32 devices in a mesh: batch: 4 (over y, x), centre: 8 (over z, core).
Axes of the slice: x: 2, y: 2, z: 4, core: 2. Of those that a mesh axis runs over, the one named last changes fastest.
Arguments:
- pool: float32 [1024, 1024], P('batch', 'centre'), may hold values from -4.5 to 4.5
- sample_index: int32 [512], P('batch'), may hold values from 0 to 255
- targets: float32 [512, 256], P('batch'), may hold values from -6 to 6
- centres: float32 [512, 1024], P(('batch', 'centre')), may hold values from -4.5 to 4.5
- coeffs: float32 [512, 256], P(('batch', 'centre')), may hold values from -6 to 6
- eigvecs: float32 [512, 1024], P(('batch', 'centre')), may hold values from -0.75 to 0.75
- eigscale: float32 [1024], replicated, may hold values from 0.1 to 0.95
Outputs:
- new_coeffs: float32 [512, 256], P(('batch', 'centre'))
The draws below stay inside these ranges and needn't reach their ends.
Inputs may be any that keep to these rules, and one draw needn't show every extreme that they name: `sample_index`: each batch row's sample lies in the block of 256 training samples held by its own batch group; the index counts within that block.
All inputs are finite; a program needn't handle non-finite values.
Results may differ from the reference program's by a relative error of at most 0.0003.
Values sent between devices are 32-bit elements; how exact they have to be, the bound alone decides.
A program may use at most 64 MiB of HBM per device.

```python
import jax
import jax.numpy as jnp
from jax import lax

FEATURES = 1024
OUTPUTS = 256
EIGEN = 1024
ROWS_DEV = 128
SAMPLES_DEV = 256
ROWS = 512
CENTRES = 512
POOL = 1024
N_BATCH = 4


def plant(array, rng, least, high):
    dims = array.shape
    place = [jax.random.randint(jax.random.fold_in(rng, axis), (), 0, dims[axis]) for axis in range(len(dims))]
    array = array.at[tuple(place)].set(least)
    longest = dims.index(max(dims))
    place[longest] = (place[longest] + 1) % dims[longest]
    return array.at[tuple(place)].set(high)


def block_scale(own_key, extent, cuts, low, top_value):
    level, own = 1.0, jax.random.fold_in(own_key, 6)
    for axis_at, shards_of in cuts:
        draws = jnp.exp(jax.random.uniform(jax.random.fold_in(own, axis_at), (shards_of,), jnp.float32, low / len(cuts), top_value / len(cuts)))
        level = level * jnp.repeat(draws, extent[axis_at] // shards_of).reshape([-1 if axis == axis_at else 1 for axis in range(len(extent))])
    return level


def bell_draw(own_key, dims, width, limit, shards=(), held_as=jnp.bfloat16):
    gain = block_scale(own_key, dims, shards, -0.22, 0.18) if shards else 1.0
    values = jax.random.normal(own_key, dims, jnp.float32) * width * gain
    return jnp.minimum(jnp.maximum(values, -limit), limit).astype(held_as)


def setup_inputs(seed: int = 0) -> dict:
    key_of = jax.random.split(jax.random.key(seed), 8)
    return {
        "pool": bell_draw(key_of[0], (POOL, FEATURES), 0.75, 4.5, ((0, 4), (1, 8)), jnp.float32),
        "sample_index": plant(jax.random.randint(key_of[1], (ROWS,), 0, SAMPLES_DEV), jax.random.fold_in(key_of[1], 1), 0, SAMPLES_DEV - 1).astype(jnp.int32),
        "targets": bell_draw(key_of[2], (ROWS, OUTPUTS), 1.0, 6.0, ((0, 4),), jnp.float32),
        "centres": bell_draw(key_of[3], (CENTRES, FEATURES), 0.75, 4.5, ((0, 32),), jnp.float32),
        "coeffs": bell_draw(key_of[4], (CENTRES, OUTPUTS), 1.0, 6.0, ((0, 32),), jnp.float32),
        "eigvecs": bell_draw(key_of[5], (CENTRES, EIGEN), (CENTRES // 8) ** -0.5, 0.75, ((0, 32),), jnp.float32),
        "eigscale": jnp.clip(jax.random.uniform(key_of[6], (EIGEN,), jnp.float32, 0.1, 0.95), 0.1, 0.95),
    }


def reference(pool, sample_index, targets, centres, coeffs, eigvecs, eigscale):
    highest = lax.Precision.HIGHEST
    owner = jnp.arange(ROWS, dtype=jnp.int32) // ROWS_DEV
    picks = (owner * SAMPLES_DEV + sample_index).astype(jnp.int32)
    batch_x = jnp.take(pool, picks, axis=0)
    inv_width = 1.0 / jnp.sqrt(jnp.float32(FEATURES))
    model_norm = 1.0 / jnp.sqrt(jnp.float32(CENTRES))
    blocks = N_BATCH
    block_rows = CENTRES // blocks
    zs = centres.reshape(blocks, block_rows, FEATURES)
    cs = coeffs.reshape(blocks, block_rows, OUTPUTS)

    def kernel_block(zblock):
        return jnp.exp(jnp.dot(batch_x, zblock.T, precision=highest, preferred_element_type=jnp.float32) * inv_width)

    def add_pred(totals, pieces):
        zblock, cblock = pieces
        return (totals + jnp.dot(kernel_block(zblock), cblock, precision=highest, preferred_element_type=jnp.float32), None)
    summed, unused = lax.scan(add_pred, jnp.zeros((ROWS, OUTPUTS), jnp.float32), (zs, cs))
    residual = summed * model_norm - targets

    def grad_block(zblock):
        return jnp.dot(kernel_block(zblock).T, residual, precision=highest, preferred_element_type=jnp.float32)
    gradient = lax.map(grad_block, zs).reshape(CENTRES, OUTPUTS) * model_norm
    coords = jnp.dot(eigvecs.T, gradient, precision=highest, preferred_element_type=jnp.float32)
    correction = jnp.dot(eigvecs, eigscale[:, None] * coords, precision=highest, preferred_element_type=jnp.float32)
    step_size = 0.5 * jnp.sqrt(jnp.float32(CENTRES) / jnp.float32(ROWS))
    return coeffs - step_size * (gradient - correction)
```

```python
import jax
import jax.numpy as jnp
from jax import lax
from jax.experimental import pallas as pl
from jax.experimental.pallas import tpu as pltpu
from jax.sharding import PartitionSpec as P

MESH = pl.DeviceIdType.MESH
F32 = jnp.float32


def mm(a, b, dims):
    return lax.dot_general(
        a, b, (dims, ((), ())), precision=lax.Precision.HIGHEST, preferred_element_type=F32
    )


def rows_of(buf):
    count, depth, width = buf.shape
    if depth % 8 == 0:
        return buf[...].reshape(count * depth, width)
    return jnp.concatenate([buf[j] for j in range(count)], axis=0)


def step_kernel(
    nb, nc, inv_width, model_norm, step_size,
    x_ref, t_ref, z_ref, a_ref, e_ref, s_ref, out_ref,
    xs, ec, zs, cs, eb, pout, pin, rs, gs, gsum, cout, cin,
    x_send, x_recv, ec_send, ec_recv, b_send, b_recv,
    p_send, p_recv, r_send, r_recv, g_send, g_recv, c_send, c_recv,
):
    b = lax.axis_index("batch")
    c = lax.axis_index("centre")
    own = z_ref.shape[0]
    part = t_ref.shape[1]
    width = x_ref.shape[1]
    mate = c + 1 - 2 * lax.rem(c, 2)
    others = [lax.rem(c + k, nc) for k in range(1, nc)]
    groups = [lax.rem(b + k, nb) for k in range(1, nb)]
    pending = []

    def push(src, dst, send, recv, bi, ci):
        copy = pltpu.make_async_remote_copy(
            src_ref=src, dst_ref=dst, send_sem=send, recv_sem=recv,
            device_id=(bi, ci), device_id_type=MESH,
        )
        copy.start()
        pending.append(copy)

    def arrived(dst, recv):
        pltpu.make_async_remote_copy(
            src_ref=dst, dst_ref=dst, send_sem=recv, recv_sem=recv,
            device_id=(b, mate), device_id_type=MESH,
        ).wait_recv()

    barrier = pltpu.get_barrier_semaphore()
    for ci in others:
        pl.semaphore_signal(barrier, inc=1, device_id=(b, ci), device_id_type=MESH)
    for bi in groups:
        pl.semaphore_signal(barrier, inc=1, device_id=(bi, c), device_id_type=MESH)
    pl.semaphore_wait(barrier, nc - 1 + nb - 1)

    half = nc // 2
    peers = [lax.rem(c + 2 * k, nc) for k in range(1, half)]
    for k, ci in enumerate(peers):
        push(x_ref, xs.at[c], x_send.at[k], x_recv.at[c], b, ci)
    push(x_ref, xs.at[c], x_send.at[half - 1], x_recv.at[c], b, mate)
    for k, bi in enumerate(groups):
        push(z_ref, zs.at[b], b_send.at[0, k], b_recv.at[0, b], bi, c)
    for k, bi in enumerate(groups):
        push(a_ref, cs.at[b], b_send.at[1, k], b_recv.at[1, b], bi, c)
    for k, ci in enumerate(peers):
        push(e_ref, ec.at[c], ec_send.at[k], ec_recv.at[c], b, ci)
    push(e_ref, ec.at[c], ec_send.at[half - 1], ec_recv.at[c], b, mate)
    for k, bi in enumerate(groups):
        push(e_ref, eb.at[b], b_send.at[2, k], b_recv.at[2, b], bi, c)
    xs[c] = x_ref[...]
    ec[c] = e_ref[...]
    zs[b] = z_ref[...]
    cs[b] = a_ref[...]
    eb[b] = e_ref[...]

    sources = [lax.rem(c + nc - 2 * k, nc) for k in range(1, half)]
    for k, ci in enumerate(sources):
        arrived(xs.at[ci], x_recv.at[ci])
        push(xs.at[ci], xs.at[ci], x_send.at[half + k], x_recv.at[ci], b, mate)
    for bi in groups:
        arrived(zs.at[bi], b_recv.at[0, bi])
    arrived(xs.at[mate], x_recv.at[mate])
    for k in range(1, half):
        ci = lax.rem(mate + nc - 2 * k, nc)
        arrived(xs.at[ci], x_recv.at[ci])

    scores = None
    for j in range(nc):
        zj = zs[:, :, j * width:(j + 1) * width].reshape(nb * own, width)
        term = mm(xs[j], zj, ((1,), (1,)))
        scores = term if scores is None else scores + term
    kernel = jnp.exp(scores * inv_width)
    for bi in groups:
        arrived(cs.at[bi], b_recv.at[1, bi])
    value = mm(kernel, rows_of(cs), ((1,), (0,)))
    for j in range(nc):
        pout[j] = value[j * part:(j + 1) * part]
    for k, ci in enumerate(others):
        push(pout.at[ci], pin.at[c], p_send.at[k], p_recv.at[c], b, ci)
    pin[c] = pout[c]

    for k, ci in enumerate(sources):
        arrived(ec.at[ci], ec_recv.at[ci])
        push(ec.at[ci], ec.at[ci], ec_send.at[half + k], ec_recv.at[ci], b, mate)

    for ci in others:
        arrived(pin.at[ci], p_recv.at[ci])
    total = pin[0]
    for j in range(1, nc):
        total = total + pin[j]
    rs[c] = total * model_norm - t_ref[c]
    for k, ci in enumerate(others):
        push(rs.at[c], rs.at[c], r_send.at[k], r_recv.at[c], b, ci)

    arrived(ec.at[mate], ec_recv.at[mate])
    for k in range(1, half):
        ci = lax.rem(mate + nc - 2 * k, nc)
        arrived(ec.at[ci], ec_recv.at[ci])
    for bi in groups:
        arrived(eb.at[bi], b_recv.at[2, bi])
    mix = mm(rows_of(ec) * s_ref[...], rows_of(eb), ((1,), (1,)))
    kernel_t = kernel.T

    for ci in others:
        arrived(rs.at[ci], r_recv.at[ci])
    gs[b] = mm(kernel_t, rows_of(rs), ((1,), (0,)))
    for k, bi in enumerate(groups):
        push(gs.at[b], gs.at[b], g_send.at[k], g_recv.at[b], bi, c)
    for bi in groups:
        arrived(gs.at[bi], g_recv.at[bi])
    grad = gs[0]
    for j in range(1, nb):
        grad = grad + gs[j]
    grad = grad * model_norm
    gsum[...] = grad.reshape(nb, own, grad.shape[1])
    moved = mm(mix, grad, ((1,), (0,)))
    for j in range(nc):
        cout[j] = moved[j * own:(j + 1) * own]
    for k, ci in enumerate(others):
        push(cout.at[ci], cin.at[c], c_send.at[k], c_recv.at[c], b, ci)
    cin[c] = cout[c]
    for ci in others:
        arrived(cin.at[ci], c_recv.at[ci])
    fix = cin[0]
    for j in range(1, nc):
        fix = fix + cin[j]
    out_ref[...] = a_ref[...] - step_size * (gsum[b] - fix)
    for copy in pending:
        copy.wait_send()


def on_device(pool, sample_index, targets, centres, coeffs, eigvecs, eigscale):
    nb = lax.axis_size("batch")
    nc = lax.axis_size("centre")
    picked = jnp.take(pool, sample_index, axis=0)
    rows, part_width = picked.shape
    own, features = centres.shape
    outputs = targets.shape[1]
    eigen = eigvecs.shape[1]
    total_centres = own * nb * nc
    part = rows // nc
    body = lambda *refs: step_kernel(
        nb, nc, features ** -0.5, total_centres ** -0.5,
        0.5 * (total_centres / (rows * nb)) ** 0.5, *refs
    )
    dma = pltpu.SemaphoreType.DMA
    vmem = lambda *dims: pltpu.VMEM(dims, F32)
    return pl.pallas_call(
        body,
        out_shape=jax.ShapeDtypeStruct((own, outputs), F32),
        in_specs=[pl.BlockSpec(memory_space=pltpu.VMEM)] * 6,
        out_specs=pl.BlockSpec(memory_space=pltpu.VMEM),
        scratch_shapes=[
            vmem(nc, rows, part_width),
            vmem(nc, own, eigen),
            vmem(nb, own, features),
            vmem(nb, own, outputs),
            vmem(nb, own, eigen),
            vmem(nc, part, outputs),
            vmem(nc, part, outputs),
            vmem(nc, part, outputs),
            vmem(nb, nb * own, outputs),
            vmem(nb, own, outputs),
            vmem(nc, own, outputs),
            vmem(nc, own, outputs),
            dma((nc,)), dma((nc,)),
            dma((nc,)), dma((nc,)),
            dma((3, nb)), dma((3, nb)),
            dma((nc,)), dma((nc,)),
            dma((nc,)), dma((nc,)),
            dma((nb,)), dma((nb,)),
            dma((nc,)), dma((nc,)),
        ],
        compiler_params=pltpu.CompilerParams(
            collective_id=0, has_side_effects=True, vmem_limit_bytes=48 * 1024 * 1024
        ),
    )(
        picked,
        targets.reshape(nc, part, outputs),
        centres,
        coeffs,
        eigvecs,
        eigscale[None, :],
    )


def solution(mesh):
    return jax.shard_map(
        on_device,
        mesh=mesh,
        in_specs=(
            P("batch", "centre"),
            P("batch"),
            P("batch", None),
            P(("batch", "centre"), None),
            P(("batch", "centre"), None),
            P(("batch", "centre"), None),
            P(),
        ),
        out_specs=P(("batch", "centre"), None),
        check_vma=False,
    )
```

```python
import jax
import jax.numpy as jnp
from jax import lax
from jax.experimental import pallas as pl
from jax.experimental.pallas import tpu as pltpu
from jax.sharding import PartitionSpec as P

MESH = pl.DeviceIdType.MESH
F32 = jnp.float32


def mm(a, b, dims):
    return lax.dot_general(
        a, b, (dims, ((), ())), precision=lax.Precision.HIGHEST, preferred_element_type=F32
    )


def rows_of(buf):
    count, depth, width = buf.shape
    if depth % 8 == 0:
        return buf[...].reshape(count * depth, width)
    return jnp.concatenate([buf[j] for j in range(count)], axis=0)


def step_kernel(
    nb, nc, inv_width, model_norm, step_size,
    pool_hbm, i_hbm, t_hbm, z_hbm, a_hbm, e_hbm, s_hbm, out_ref,
    pool_ref, i_ref, t_ref, s_ref, zcol, local, xs, ec, zs, cs, eb, pout, pin, rs, gs, gsum, cout, cin,
    x_send, x_recv, ec_send, ec_recv, b_send, b_recv,
    p_send, p_recv, r_send, r_recv, g_send, g_recv, c_send, c_recv,
):
    b = lax.axis_index("batch")
    c = lax.axis_index("centre")
    own = z_hbm.shape[0]
    part = t_hbm.shape[1]
    width = pool_hbm.shape[1]
    mate = c + 1 - 2 * lax.rem(c, 2)
    others = [lax.rem(c + k, nc) for k in range(1, nc)]
    groups = [lax.rem(b + k, nb) for k in range(1, nb)]
    pending = []

    def push(src, dst, send, recv, bi, ci):
        copy = pltpu.make_async_remote_copy(
            src_ref=src, dst_ref=dst, send_sem=send, recv_sem=recv,
            device_id=(bi, ci), device_id_type=MESH,
        )
        copy.start()
        pending.append(copy)

    def arrived(dst, recv):
        pltpu.make_async_remote_copy(
            src_ref=dst, dst_ref=dst, send_sem=recv, recv_sem=recv,
            device_id=(b, mate), device_id_type=MESH,
        ).wait_recv()

    barrier = pltpu.get_barrier_semaphore()
    for ci in others:
        pl.semaphore_signal(barrier, inc=1, device_id=(b, ci), device_id_type=MESH)
    for bi in groups:
        pl.semaphore_signal(barrier, inc=1, device_id=(bi, c), device_id_type=MESH)
    fetches = []
    for k, (src, dst) in enumerate([
        (pool_hbm, pool_ref), (i_hbm, i_ref), (z_hbm, zs.at[b]), (a_hbm, cs.at[b]),
        (e_hbm, ec.at[c]), (e_hbm, eb.at[b]), (s_hbm, s_ref), (t_hbm.at[c], t_ref),
    ]):
        copy = pltpu.make_async_copy(src, dst, local.at[k])
        copy.start()
        fetches.append(copy)
    fetches[0].wait()
    fetches[1].wait()
    rows = i_ref.shape[1]
    lines = lax.broadcasted_iota(jnp.int32, (pool_ref.shape[0], rows), 0)
    chosen = jnp.where(lines == i_ref[...], 1.0, 0.0).astype(F32)
    xs[c] = mm(chosen, pool_ref[...], ((0,), (0,)))
    for copy in fetches[2:]:
        copy.wait()
    pl.semaphore_wait(barrier, nc - 1 + nb - 1)

    half = nc // 2
    peers = [lax.rem(c + 2 * k, nc) for k in range(1, half)]
    for k, ci in enumerate(peers):
        push(xs.at[c], xs.at[c], x_send.at[k], x_recv.at[c], b, ci)
    push(xs.at[c], xs.at[c], x_send.at[half - 1], x_recv.at[c], b, mate)
    for k, bi in enumerate(groups):
        push(zs.at[b], zs.at[b], b_send.at[0, k], b_recv.at[0, b], bi, c)
    for k, bi in enumerate(groups):
        push(cs.at[b], cs.at[b], b_send.at[1, k], b_recv.at[1, b], bi, c)
    for k, ci in enumerate(peers):
        push(ec.at[c], ec.at[c], ec_send.at[k], ec_recv.at[c], b, ci)
    push(ec.at[c], ec.at[c], ec_send.at[half - 1], ec_recv.at[c], b, mate)
    for k, bi in enumerate(groups):
        push(eb.at[b], eb.at[b], b_send.at[2, k], b_recv.at[2, b], bi, c)

    sources = [lax.rem(c + nc - 2 * k, nc) for k in range(1, half)]
    for bi in groups:
        arrived(zs.at[bi], b_recv.at[0, bi])
    for j in range(nc):
        zcol[j] = zs[:, :, j * width:(j + 1) * width].reshape(nb * own, width)
    scores = mm(xs[c], zcol[c], ((1,), (1,)))
    arrived(xs.at[mate], x_recv.at[mate])
    scores = scores + mm(xs[mate], zcol[mate], ((1,), (1,)))
    for k, ci in enumerate(sources):
        arrived(xs.at[ci], x_recv.at[ci])
        push(xs.at[ci], xs.at[ci], x_send.at[half + k], x_recv.at[ci], b, mate)
        scores = scores + mm(xs[ci], zcol[ci], ((1,), (1,)))
    for k in range(1, half):
        ci = lax.rem(mate + nc - 2 * k, nc)
        arrived(xs.at[ci], x_recv.at[ci])
        scores = scores + mm(xs[ci], zcol[ci], ((1,), (1,)))
    kernel = jnp.exp(scores * inv_width)
    for bi in groups:
        arrived(cs.at[bi], b_recv.at[1, bi])
    value = mm(kernel, rows_of(cs), ((1,), (0,)))
    for j in range(nc):
        pout[j] = value[j * part:(j + 1) * part]
    for k, ci in enumerate(others):
        push(pout.at[ci], pin.at[c], p_send.at[k], p_recv.at[c], b, ci)
    pin[c] = pout[c]

    for k, ci in enumerate(sources):
        arrived(ec.at[ci], ec_recv.at[ci])
        push(ec.at[ci], ec.at[ci], ec_send.at[half + k], ec_recv.at[ci], b, mate)

    for ci in others:
        arrived(pin.at[ci], p_recv.at[ci])
    total = pin[0]
    for j in range(1, nc):
        total = total + pin[j]
    rs[c] = total * model_norm - t_ref[...]
    for k, ci in enumerate(others):
        push(rs.at[c], rs.at[c], r_send.at[k], r_recv.at[c], b, ci)

    arrived(ec.at[mate], ec_recv.at[mate])
    for k in range(1, half):
        ci = lax.rem(mate + nc - 2 * k, nc)
        arrived(ec.at[ci], ec_recv.at[ci])
    for bi in groups:
        arrived(eb.at[bi], b_recv.at[2, bi])
    mix = mm(rows_of(ec) * s_ref[...], rows_of(eb), ((1,), (1,)))
    kernel_t = kernel.T

    for ci in others:
        arrived(rs.at[ci], r_recv.at[ci])
    gs[b] = mm(kernel_t, rows_of(rs), ((1,), (0,)))
    for k, bi in enumerate(groups):
        push(gs.at[b], gs.at[b], g_send.at[k], g_recv.at[b], bi, c)
    for bi in groups:
        arrived(gs.at[bi], g_recv.at[bi])
    grad = gs[0]
    for j in range(1, nb):
        grad = grad + gs[j]
    grad = grad * model_norm
    gsum[...] = grad.reshape(nb, own, grad.shape[1])
    moved = mm(mix, grad, ((1,), (0,)))
    for j in range(nc):
        cout[j] = moved[j * own:(j + 1) * own]
    for k, ci in enumerate(others):
        push(cout.at[ci], cin.at[c], c_send.at[k], c_recv.at[c], b, ci)
    cin[c] = cout[c]
    for ci in others:
        arrived(cin.at[ci], c_recv.at[ci])
    fix = cin[0]
    for j in range(1, nc):
        fix = fix + cin[j]
    out_ref[...] = cs[b] - step_size * (gsum[b] - fix)
    for copy in pending:
        copy.wait_send()


def on_device(pool, sample_index, targets, centres, coeffs, eigvecs, eigscale):
    nb = lax.axis_size("batch")
    nc = lax.axis_size("centre")
    rows = sample_index.shape[0]
    part_width = pool.shape[1]
    own, features = centres.shape
    outputs = targets.shape[1]
    eigen = eigvecs.shape[1]
    total_centres = own * nb * nc
    part = rows // nc
    body = lambda *refs: step_kernel(
        nb, nc, features ** -0.5, total_centres ** -0.5,
        0.5 * (total_centres / (rows * nb)) ** 0.5, *refs
    )
    dma = pltpu.SemaphoreType.DMA
    vmem = lambda *dims: pltpu.VMEM(dims, F32)
    return pl.pallas_call(
        body,
        out_shape=jax.ShapeDtypeStruct((own, outputs), F32),
        in_specs=[pl.BlockSpec(memory_space=pltpu.HBM)] * 7,
        out_specs=pl.BlockSpec(memory_space=pltpu.VMEM),
        scratch_shapes=[
            vmem(*pool.shape),
            pltpu.VMEM((1, rows), jnp.int32),
            vmem(part, outputs),
            vmem(1, eigen),
            vmem(nc, nb * own, part_width),
            dma((8,)),
            vmem(nc, rows, part_width),
            vmem(nc, own, eigen),
            vmem(nb, own, features),
            vmem(nb, own, outputs),
            vmem(nb, own, eigen),
            vmem(nc, part, outputs),
            vmem(nc, part, outputs),
            vmem(nc, part, outputs),
            vmem(nb, nb * own, outputs),
            vmem(nb, own, outputs),
            vmem(nc, own, outputs),
            vmem(nc, own, outputs),
            dma((nc,)), dma((nc,)),
            dma((nc,)), dma((nc,)),
            dma((3, nb)), dma((3, nb)),
            dma((nc,)), dma((nc,)),
            dma((nc,)), dma((nc,)),
            dma((nb,)), dma((nb,)),
            dma((nc,)), dma((nc,)),
        ],
        compiler_params=pltpu.CompilerParams(
            collective_id=0, has_side_effects=True, vmem_limit_bytes=67043328
        ),
    )(
        pool,
        sample_index[None, :],
        targets.reshape(nc, part, outputs),
        centres,
        coeffs,
        eigvecs,
        eigscale[None, :],
    )


def solution(mesh):
    return jax.shard_map(
        on_device,
        mesh=mesh,
        in_specs=(
            P("batch", "centre"),
            P("batch"),
            P("batch", None),
            P(("batch", "centre"), None),
            P(("batch", "centre"), None),
            P(("batch", "centre"), None),
            P(),
        ),
        out_specs=P(("batch", "centre"), None),
        check_vma=False,
    )
```

```python
import jax
import jax.numpy as jnp
from jax import lax
from jax.experimental import pallas as pl
from jax.experimental.pallas import tpu as pltpu
from jax.sharding import PartitionSpec as P

MESH = pl.DeviceIdType.MESH
F32 = jnp.float32


def mm(a, b, dims):
    return lax.dot_general(
        a, b, (dims, ((), ())), precision=lax.Precision.HIGHEST, preferred_element_type=F32
    )


def halves(a):
    high = a.astype(jnp.bfloat16)
    return high, (a - high.astype(F32)).astype(jnp.bfloat16)


def mm3(left, right):
    dot = lambda a, b: jnp.dot(a, b, preferred_element_type=F32)
    (ah, al), (bh, bl) = left, right
    return dot(ah, bh) + (dot(ah, bl) + dot(al, bh))


def rows_of(buf):
    count, depth, width = buf.shape
    if depth % 8 == 0:
        return buf[...].reshape(count * depth, width)
    return jnp.concatenate([buf[j] for j in range(count)], axis=0)


def step_kernel(
    nb, nc, inv_width, model_norm,
    pool_hbm, i_hbm, t_hbm, z_hbm, a_hbm, e_hbm, s_hbm, out_ref,
    pool_ref, i_ref, t_ref, s_ref, zcol, local, xs, ec, zs, cs, eb, pout, pin, rs, gs, gsum, cout, cin,
    x_send, x_recv, ec_send, ec_recv, b_send, b_recv,
    p_send, p_recv, r_send, r_recv, g_send, g_recv, c_send, c_recv,
):
    b = lax.axis_index("batch")
    c = lax.axis_index("centre")
    own = z_hbm.shape[0]
    part = t_hbm.shape[1]
    width = pool_hbm.shape[1]
    mate = c + 1 - 2 * lax.rem(c, 2)
    others = [lax.rem(c + k, nc) for k in range(1, nc)]
    groups = [lax.rem(b + k, nb) for k in range(1, nb)]
    pending = []

    def push(src, dst, send, recv, bi, ci):
        copy = pltpu.make_async_remote_copy(
            src_ref=src, dst_ref=dst, send_sem=send, recv_sem=recv,
            device_id=(bi, ci), device_id_type=MESH,
        )
        copy.start()
        pending.append(copy)

    def arrived(dst, recv):
        pltpu.make_async_remote_copy(
            src_ref=dst, dst_ref=dst, send_sem=recv, recv_sem=recv,
            device_id=(b, mate), device_id_type=MESH,
        ).wait_recv()

    barrier = pltpu.get_barrier_semaphore()
    for ci in others:
        pl.semaphore_signal(barrier, inc=1, device_id=(b, ci), device_id_type=MESH)
    for bi in groups:
        pl.semaphore_signal(barrier, inc=1, device_id=(bi, c), device_id_type=MESH)
    fetches = []
    for k, (src, dst) in enumerate([
        (pool_hbm, pool_ref), (i_hbm, i_ref), (z_hbm, zs.at[b]), (a_hbm, cs.at[b]),
        (e_hbm, ec.at[c]), (e_hbm, eb.at[b]), (s_hbm, s_ref), (t_hbm.at[c], t_ref),
    ]):
        copy = pltpu.make_async_copy(src, dst, local.at[k])
        copy.start()
        fetches.append(copy)
    fetches[0].wait()
    fetches[1].wait()
    rows = i_ref.shape[1]
    lines = lax.broadcasted_iota(jnp.int32, (pool_ref.shape[0], rows), 0)
    chosen = jnp.where(lines == i_ref[...], 1.0, 0.0).astype(F32)
    xs[c] = mm(chosen, pool_ref[...], ((0,), (0,)))
    for copy in fetches[2:]:
        copy.wait()
    pl.semaphore_wait(barrier, nc - 1 + nb - 1)

    half = nc // 2
    peers = [lax.rem(c + 2 * k, nc) for k in range(1, half)]
    for k, ci in enumerate(peers):
        push(xs.at[c], xs.at[c], x_send.at[k], x_recv.at[c], b, ci)
    push(xs.at[c], xs.at[c], x_send.at[half - 1], x_recv.at[c], b, mate)
    for k, bi in enumerate(groups):
        push(zs.at[b], zs.at[b], b_send.at[0, k], b_recv.at[0, b], bi, c)
    for k, bi in enumerate(groups):
        push(cs.at[b], cs.at[b], b_send.at[1, k], b_recv.at[1, b], bi, c)
    for k, ci in enumerate(peers):
        push(ec.at[c], ec.at[c], ec_send.at[k], ec_recv.at[c], b, ci)
    push(ec.at[c], ec.at[c], ec_send.at[half - 1], ec_recv.at[c], b, mate)
    for k, bi in enumerate(groups):
        push(eb.at[b], eb.at[b], b_send.at[2, k], b_recv.at[2, b], bi, c)

    sources = [lax.rem(c + nc - 2 * k, nc) for k in range(1, half)]
    for bi in groups:
        arrived(zs.at[bi], b_recv.at[0, bi])
    for j in range(nc):
        zcol[j] = zs[:, :, j * width:(j + 1) * width].reshape(nb * own, width)
    for bi in groups:
        arrived(cs.at[bi], b_recv.at[1, bi])
    weights = halves(rows_of(cs))
    scores = mm(xs[c], zcol[c], ((1,), (1,)))
    arrived(xs.at[mate], x_recv.at[mate])
    scores = scores + mm(xs[mate], zcol[mate], ((1,), (1,)))
    for k, ci in enumerate(sources):
        arrived(xs.at[ci], x_recv.at[ci])
        push(xs.at[ci], xs.at[ci], x_send.at[half + k], x_recv.at[ci], b, mate)
        scores = scores + mm(xs[ci], zcol[ci], ((1,), (1,)))
    for k in range(1, half):
        ci = lax.rem(mate + nc - 2 * k, nc)
        arrived(xs.at[ci], x_recv.at[ci])
        scores = scores + mm(xs[ci], zcol[ci], ((1,), (1,)))
    kernel = jnp.exp(scores * inv_width)
    value = mm3(halves(kernel), weights)
    for j in range(nc):
        pout[j] = value[j * part:(j + 1) * part]
    for k, ci in enumerate(others):
        push(pout.at[ci], pin.at[c], p_send.at[k], p_recv.at[c], b, ci)
    pin[c] = pout[c]

    for k, ci in enumerate(sources):
        arrived(ec.at[ci], ec_recv.at[ci])
        push(ec.at[ci], ec.at[ci], ec_send.at[half + k], ec_recv.at[ci], b, mate)

    for ci in others:
        arrived(pin.at[ci], p_recv.at[ci])
    total = pin[0]
    for j in range(1, nc):
        total = total + pin[j]
    rs[c] = total * model_norm - t_ref[...]
    for k, ci in enumerate(others):
        push(rs.at[c], rs.at[c], r_send.at[k], r_recv.at[c], b, ci)

    arrived(ec.at[mate], ec_recv.at[mate])
    for k in range(1, half):
        ci = lax.rem(mate + nc - 2 * k, nc)
        arrived(ec.at[ci], ec_recv.at[ci])
    for bi in groups:
        arrived(eb.at[bi], b_recv.at[2, bi])
    mix = halves(mm(rows_of(ec) * s_ref[...], rows_of(eb), ((1,), (1,))))
    kernel_t = halves(kernel.T)

    for ci in others:
        arrived(rs.at[ci], r_recv.at[ci])
    gs[b] = mm3(kernel_t, halves(rows_of(rs)))
    for k, bi in enumerate(groups):
        push(gs.at[b], gs.at[b], g_send.at[k], g_recv.at[b], bi, c)
    for bi in groups:
        arrived(gs.at[bi], g_recv.at[bi])
    grad = gs[0]
    for j in range(1, nb):
        grad = grad + gs[j]
    grad = grad * model_norm
    gsum[...] = grad.reshape(nb, own, grad.shape[1])
    moved = mm3(mix, halves(grad))
    for j in range(nc):
        cout[j] = moved[j * own:(j + 1) * own]
    for k, ci in enumerate(others):
        push(cout.at[ci], cin.at[c], c_send.at[k], c_recv.at[c], b, ci)
    cin[c] = cout[c]
    for ci in others:
        arrived(cin.at[ci], c_recv.at[ci])
    fix = cin[0]
    for j in range(1, nc):
        fix = fix + cin[j]
    out_ref[...] = gsum[b] - fix
    for copy in pending:
        copy.wait_send()


def on_device(pool, sample_index, targets, centres, coeffs, eigvecs, eigscale):
    nb = lax.axis_size("batch")
    nc = lax.axis_size("centre")
    rows = sample_index.shape[0]
    part_width = pool.shape[1]
    own, features = centres.shape
    outputs = targets.shape[1]
    eigen = eigvecs.shape[1]
    total_centres = own * nb * nc
    part = rows // nc
    body = lambda *refs: step_kernel(
        nb, nc, features ** -0.5, total_centres ** -0.5, *refs
    )
    dma = pltpu.SemaphoreType.DMA
    vmem = lambda *dims: pltpu.VMEM(dims, F32)
    delta = pl.pallas_call(
        body,
        out_shape=jax.ShapeDtypeStruct((own, outputs), F32),
        in_specs=[pl.BlockSpec(memory_space=pltpu.HBM)] * 7,
        out_specs=pl.BlockSpec(memory_space=pltpu.VMEM),
        scratch_shapes=[
            vmem(*pool.shape),
            pltpu.VMEM((1, rows), jnp.int32),
            vmem(part, outputs),
            vmem(1, eigen),
            vmem(nc, nb * own, part_width),
            dma((8,)),
            vmem(nc, rows, part_width),
            vmem(nc, own, eigen),
            vmem(nb, own, features),
            vmem(nb, own, outputs),
            vmem(nb, own, eigen),
            vmem(nc, part, outputs),
            vmem(nc, part, outputs),
            vmem(nc, part, outputs),
            vmem(nb, nb * own, outputs),
            vmem(nb, own, outputs),
            vmem(nc, own, outputs),
            vmem(nc, own, outputs),
            dma((nc,)), dma((nc,)),
            dma((nc,)), dma((nc,)),
            dma((3, nb)), dma((3, nb)),
            dma((nc,)), dma((nc,)),
            dma((nc,)), dma((nc,)),
            dma((nb,)), dma((nb,)),
            dma((nc,)), dma((nc,)),
        ],
        compiler_params=pltpu.CompilerParams(
            collective_id=0, has_side_effects=True, vmem_limit_bytes=67043328
        ),
    )(
        pool,
        sample_index[None, :],
        targets.reshape(nc, part, outputs),
        centres,
        coeffs,
        eigvecs,
        eigscale[None, :],
    )
    return coeffs - 0.5 * (total_centres / (rows * nb)) ** 0.5 * delta


def solution(mesh):
    return jax.shard_map(
        on_device,
        mesh=mesh,
        in_specs=(
            P("batch", "centre"),
            P("batch"),
            P("batch", None),
            P(("batch", "centre"), None),
            P(("batch", "centre"), None),
            P(("batch", "centre"), None),
            P(),
        ),
        out_specs=P(("batch", "centre"), None),
        check_vma=False,
    )
```

```python
import jax
import jax.numpy as jnp
from jax import lax
from jax.experimental import pallas as pl
from jax.experimental.pallas import tpu as pltpu
from jax.sharding import PartitionSpec as P

MESH = pl.DeviceIdType.MESH
F32 = jnp.float32


def mm(a, b, dims):
    return lax.dot_general(
        a, b, (dims, ((), ())), precision=lax.Precision.HIGHEST, preferred_element_type=F32
    )


def farthest_first(z, n):
    side = z // (n // 2)
    near = z + side * (n - 1 - 2 * z)
    lone = n - 1 - 2 * near
    order = []
    for k in range(n - 1):
        paired = (k - lone + n) // n
        step = paired * (k - lone)
        beyond = near + (1 - 2 * (step % 2)) * (near - step // 2)
        chip = (1 - paired) * (n - 1 - k) + paired * beyond
        order.append(chip + side * (n - 1 - 2 * chip))
    return order


def flipped(b, k):
    bit = 1
    while bit <= k:
        if k & bit:
            b = b + bit * (1 - 2 * ((b // bit) % 2))
        bit *= 2
    return b


def rows_of(buf):
    count, depth, width = buf.shape
    if depth % 8 == 0:
        return buf[...].reshape(count * depth, width)
    return jnp.concatenate([buf[j] for j in range(count)], axis=0)


def step_kernel(
    nb, nc, inv_width, model_norm, step_size,
    pool_hbm, i_hbm, t_hbm, z_hbm, a_hbm, e_hbm, s_hbm, out_ref,
    pool_ref, i_ref, t_ref, s_ref, zcol, local, xs, ec, zs, cs, eb, pout, pin, rs, gs, gsum, cout, cin,
    x_send, x_recv, ec_send, ec_recv, b_send, b_recv,
    p_send, p_recv, r_send, r_recv, g_send, g_recv, c_send, c_recv,
):
    b = lax.axis_index("batch")
    c = lax.axis_index("centre")
    own = z_hbm.shape[0]
    part = t_hbm.shape[1]
    width = pool_hbm.shape[1]
    mate = c + 1 - 2 * lax.rem(c, 2)
    core = lax.rem(c, 2)
    half = nc // 2
    chips = farthest_first(c // 2, half)
    peers = [2 * chip + core for chip in chips]
    others = [2 * chip + side for chip in chips for side in (core, 1 - core)] + [mate]
    if nb & (nb - 1):
        groups = [lax.rem(b + k, nb) for k in range(1, nb)]
    else:
        groups = [flipped(b, k) for k in range(nb - 1, 0, -1)]
    pending = []

    def push(src, dst, send, recv, bi, ci):
        copy = pltpu.make_async_remote_copy(
            src_ref=src, dst_ref=dst, send_sem=send, recv_sem=recv,
            device_id=(bi, ci), device_id_type=MESH,
        )
        copy.start()
        pending.append(copy)

    def arrived(dst, recv):
        pltpu.make_async_remote_copy(
            src_ref=dst, dst_ref=dst, send_sem=recv, recv_sem=recv,
            device_id=(b, mate), device_id_type=MESH,
        ).wait_recv()

    barrier = pltpu.get_barrier_semaphore()
    for ci in others:
        pl.semaphore_signal(barrier, inc=1, device_id=(b, ci), device_id_type=MESH)
    for bi in groups:
        pl.semaphore_signal(barrier, inc=1, device_id=(bi, c), device_id_type=MESH)
    fetches = []
    for k, (src, dst) in enumerate([
        (pool_hbm, pool_ref), (i_hbm, i_ref), (z_hbm, zs.at[b]), (a_hbm, cs.at[b]),
        (e_hbm, ec.at[c]), (e_hbm, eb.at[b]), (s_hbm, s_ref), (t_hbm.at[c], t_ref),
    ]):
        copy = pltpu.make_async_copy(src, dst, local.at[k])
        copy.start()
        fetches.append(copy)
    fetches[0].wait()
    fetches[1].wait()
    rows = i_ref.shape[1]
    lines = lax.broadcasted_iota(jnp.int32, (pool_ref.shape[0], rows), 0)
    chosen = jnp.where(lines == i_ref[...], 1.0, 0.0).astype(F32)
    xs[c] = mm(chosen, pool_ref[...], ((0,), (0,)))
    for copy in fetches[2:]:
        copy.wait()
    pl.semaphore_wait(barrier, nc - 1 + nb - 1)

    for k, ci in enumerate(peers):
        push(xs.at[c], xs.at[c], x_send.at[k], x_recv.at[c], b, ci)
    push(xs.at[c], xs.at[c], x_send.at[half - 1], x_recv.at[c], b, mate)
    for k, bi in enumerate(groups):
        push(zs.at[b], zs.at[b], b_send.at[0, k], b_recv.at[0, b], bi, c)
    for k, bi in enumerate(groups):
        push(cs.at[b], cs.at[b], b_send.at[1, k], b_recv.at[1, b], bi, c)
    for k, ci in enumerate(peers):
        push(ec.at[c], ec.at[c], ec_send.at[k], ec_recv.at[c], b, ci)
    push(ec.at[c], ec.at[c], ec_send.at[half - 1], ec_recv.at[c], b, mate)
    for k, bi in enumerate(groups):
        push(eb.at[b], eb.at[b], b_send.at[2, k], b_recv.at[2, b], bi, c)

    for bi in groups:
        arrived(zs.at[bi], b_recv.at[0, bi])
    for j in range(nc):
        zcol[j] = zs[:, :, j * width:(j + 1) * width].reshape(nb * own, width)
    scores = mm(xs[c], zcol[c], ((1,), (1,)))
    arrived(xs.at[mate], x_recv.at[mate])
    scores = scores + mm(xs[mate], zcol[mate], ((1,), (1,)))
    for k, ci in enumerate(peers):
        arrived(xs.at[ci], x_recv.at[ci])
        push(xs.at[ci], xs.at[ci], x_send.at[half + k], x_recv.at[ci], b, mate)
        scores = scores + mm(xs[ci], zcol[ci], ((1,), (1,)))
    for ci in [2 * chip + 1 - core for chip in chips]:
        arrived(xs.at[ci], x_recv.at[ci])
        scores = scores + mm(xs[ci], zcol[ci], ((1,), (1,)))
    kernel = jnp.exp(scores * inv_width)
    for bi in groups:
        arrived(cs.at[bi], b_recv.at[1, bi])
    value = mm(kernel, rows_of(cs), ((1,), (0,)))
    for j in range(nc):
        pout[j] = value[j * part:(j + 1) * part]
    for k, ci in enumerate(others):
        push(pout.at[ci], pin.at[c], p_send.at[k], p_recv.at[c], b, ci)
    pin[c] = pout[c]

    for k, ci in enumerate(peers):
        arrived(ec.at[ci], ec_recv.at[ci])
        push(ec.at[ci], ec.at[ci], ec_send.at[half + k], ec_recv.at[ci], b, mate)

    for ci in others:
        arrived(pin.at[ci], p_recv.at[ci])
    total = pin[0]
    for j in range(1, nc):
        total = total + pin[j]
    rs[c] = total * model_norm - t_ref[...]
    for k, ci in enumerate(others):
        push(rs.at[c], rs.at[c], r_send.at[k], r_recv.at[c], b, ci)

    arrived(ec.at[mate], ec_recv.at[mate])
    for ci in [2 * chip + 1 - core for chip in chips]:
        arrived(ec.at[ci], ec_recv.at[ci])
    for bi in groups:
        arrived(eb.at[bi], b_recv.at[2, bi])
    mix = mm(rows_of(ec) * s_ref[...], rows_of(eb), ((1,), (1,)))
    kernel_t = kernel.T

    for ci in others:
        arrived(rs.at[ci], r_recv.at[ci])
    gs[b] = mm(kernel_t, rows_of(rs), ((1,), (0,)))
    for k, bi in enumerate(groups):
        push(gs.at[b], gs.at[b], g_send.at[k], g_recv.at[b], bi, c)
    for bi in groups:
        arrived(gs.at[bi], g_recv.at[bi])
    grad = gs[0]
    for j in range(1, nb):
        grad = grad + gs[j]
    grad = grad * model_norm
    gsum[...] = grad.reshape(nb, own, grad.shape[1])
    moved = mm(mix, grad, ((1,), (0,)))
    for j in range(nc):
        cout[j] = moved[j * own:(j + 1) * own]
    for k, ci in enumerate(others):
        push(cout.at[ci], cin.at[c], c_send.at[k], c_recv.at[c], b, ci)
    cin[c] = cout[c]
    for ci in others:
        arrived(cin.at[ci], c_recv.at[ci])
    fix = cin[0]
    for j in range(1, nc):
        fix = fix + cin[j]
    out_ref[...] = cs[b] - step_size * (gsum[b] - fix)
    for copy in pending:
        copy.wait_send()


def on_device(pool, sample_index, targets, centres, coeffs, eigvecs, eigscale):
    nb = lax.axis_size("batch")
    nc = lax.axis_size("centre")
    rows = sample_index.shape[0]
    part_width = pool.shape[1]
    own, features = centres.shape
    outputs = targets.shape[1]
    eigen = eigvecs.shape[1]
    total_centres = own * nb * nc
    part = rows // nc
    body = lambda *refs: step_kernel(
        nb, nc, features ** -0.5, total_centres ** -0.5,
        0.5 * (total_centres / (rows * nb)) ** 0.5, *refs
    )
    dma = pltpu.SemaphoreType.DMA
    vmem = lambda *dims: pltpu.VMEM(dims, F32)
    return pl.pallas_call(
        body,
        out_shape=jax.ShapeDtypeStruct((own, outputs), F32),
        in_specs=[pl.BlockSpec(memory_space=pltpu.HBM)] * 7,
        out_specs=pl.BlockSpec(memory_space=pltpu.VMEM),
        scratch_shapes=[
            vmem(*pool.shape),
            pltpu.VMEM((1, rows), jnp.int32),
            vmem(part, outputs),
            vmem(1, eigen),
            vmem(nc, nb * own, part_width),
            dma((8,)),
            vmem(nc, rows, part_width),
            vmem(nc, own, eigen),
            vmem(nb, own, features),
            vmem(nb, own, outputs),
            vmem(nb, own, eigen),
            vmem(nc, part, outputs),
            vmem(nc, part, outputs),
            vmem(nc, part, outputs),
            vmem(nb, nb * own, outputs),
            vmem(nb, own, outputs),
            vmem(nc, own, outputs),
            vmem(nc, own, outputs),
            dma((nc,)), dma((nc,)),
            dma((nc,)), dma((nc,)),
            dma((3, nb)), dma((3, nb)),
            dma((nc,)), dma((nc,)),
            dma((nc,)), dma((nc,)),
            dma((nb,)), dma((nb,)),
            dma((nc,)), dma((nc,)),
        ],
        compiler_params=pltpu.CompilerParams(
            collective_id=0, has_side_effects=True, vmem_limit_bytes=67043328
        ),
    )(
        pool,
        sample_index[None, :],
        targets.reshape(nc, part, outputs),
        centres,
        coeffs,
        eigvecs,
        eigscale[None, :],
    )


def solution(mesh):
    return jax.shard_map(
        on_device,
        mesh=mesh,
        in_specs=(
            P("batch", "centre"),
            P("batch"),
            P("batch", None),
            P(("batch", "centre"), None),
            P(("batch", "centre"), None),
            P(("batch", "centre"), None),
            P(),
        ),
        out_specs=P(("batch", "centre"), None),
        check_vma=False,
    )
```
